8 devices in a mesh: data: 2 (over z, y), model: 4 (over x, core).
Axes of the slice: x: 2, y: 2, z: 1, core: 2. Of those that a mesh axis runs over, the one named last changes fastest.
Arguments:
- x_in: bfloat16 [128, 6144], P(('data', 'model')), parts along dimension 0
- dy_in: bfloat16 [128, 6144], P(('data', 'model')), parts along dimension 0
- w_query: bfloat16 [6144, 48, 128], P(None, 'model')
- w_key: bfloat16 [6144, 128], replicated
- w_value: bfloat16 [6144, 128], replicated
- w_out: bfloat16 [48, 128, 6144], P('model')
Outputs:
- output 1: bfloat16 [128, 6144], P(('data', 'model')), parts along dimension 0
- output 2: float32 [12288, 48, 128], P('data', 'model'), parts along dimension 0
- output 3: float32 [12288, 128], P(('data', 'model')), parts along dimension 0
- output 4: float32 [12288, 128], P(('data', 'model')), parts along dimension 0
- output 5: float32 [96, 128, 6144], P(('data', 'model')), parts along dimension 0
There are 2 independent parts. The reference program is written for one: setup_inputs(seed, part) draws one part's arguments, and reference() takes and returns one part's arrays. A program takes and returns all parts, laid end to end along the dimension named above; an argument that names none is the same for every part.
All inputs are finite; a program needn't handle non-finite values.
Results may differ from the reference program's by a relative error of at most 0.0107.
Values are sent between devices in bfloat16 or wider.
A program may use at most 1 GiB of HBM per device.

```python
import math
import jax
import jax.numpy as jnp
from jax import lax

SEQ_LEN = 64
D_MODEL = 6144
NUM_HEADS = 48
HEAD_DIM = 128


def setup_inputs(seed: int = 0, part: int = 0) -> dict:
    part_key = jax.random.fold_in(jax.random.key(seed), part)
    act_keys = jax.random.split(part_key, 2)
    weight_keys = jax.random.split(jax.random.key(seed + 1), 4)
    in_scale = D_MODEL ** -0.5
    x_in = jax.random.normal(act_keys[0], (SEQ_LEN, D_MODEL), jnp.float32).astype(jnp.bfloat16)
    dy_in = jax.random.normal(act_keys[1], (SEQ_LEN, D_MODEL), jnp.float32).astype(jnp.bfloat16)
    w_query = (jax.random.normal(weight_keys[0], (D_MODEL, NUM_HEADS, HEAD_DIM), jnp.float32) * in_scale).astype(jnp.bfloat16)
    w_key = (jax.random.normal(weight_keys[1], (D_MODEL, HEAD_DIM), jnp.float32) * in_scale).astype(jnp.bfloat16)
    w_value = (jax.random.normal(weight_keys[2], (D_MODEL, HEAD_DIM), jnp.float32) * in_scale).astype(jnp.bfloat16)
    w_out = (jax.random.normal(weight_keys[3], (NUM_HEADS, HEAD_DIM, D_MODEL), jnp.float32) * in_scale).astype(jnp.bfloat16)
    return {"x_in": x_in, "dy_in": dy_in, "w_query": w_query, "w_key": w_key, "w_value": w_value, "w_out": w_out}


def reference(x_in, dy_in, w_query, w_key, w_value, w_out):
    score_scale = 1.0 / math.sqrt(HEAD_DIM)
    keys_all = jnp.dot(x_in, w_key, preferred_element_type=jnp.float32).astype(jnp.bfloat16)
    values_all = jnp.dot(x_in, w_value, preferred_element_type=jnp.float32).astype(jnp.bfloat16)
    causal = jnp.arange(SEQ_LEN)[:, None] >= jnp.arange(SEQ_LEN)[None, :]

    def head_step(carry_in, head_weights):
        dk_sum, dv_sum, dx_sum = carry_in
        wq_head, wo_head = head_weights
        query_rows = jnp.dot(x_in, wq_head, preferred_element_type=jnp.float32).astype(jnp.bfloat16)
        scores = jnp.dot(query_rows, keys_all.T, preferred_element_type=jnp.float32) * score_scale
        scores = jnp.where(causal, scores, -jnp.inf)
        probs_f32 = jax.nn.softmax(scores, axis=-1)
        probs_bf = probs_f32.astype(jnp.bfloat16)
        attn_rows = jnp.dot(probs_bf, values_all, preferred_element_type=jnp.float32).astype(jnp.bfloat16)
        dw_out_head = jnp.dot(attn_rows.T, dy_in, preferred_element_type=jnp.float32)
        d_attn = jnp.dot(dy_in, wo_head.T, preferred_element_type=jnp.float32).astype(jnp.bfloat16)
        d_probs = jnp.dot(d_attn, values_all.T, preferred_element_type=jnp.float32)
        row_dot = jnp.sum(d_attn.astype(jnp.float32) * attn_rows.astype(jnp.float32), axis=-1, keepdims=True)
        d_scores = (probs_f32 * (d_probs - row_dot) * score_scale).astype(jnp.bfloat16)
        d_query = jnp.dot(d_scores, keys_all, preferred_element_type=jnp.float32).astype(jnp.bfloat16)
        d_keys_part = jnp.dot(d_scores.T, query_rows, preferred_element_type=jnp.float32)
        d_values_part = jnp.dot(probs_bf.T, d_attn, preferred_element_type=jnp.float32)
        dw_query_head = jnp.dot(x_in.T, d_query, preferred_element_type=jnp.float32)
        dx_part = jnp.dot(d_query, wq_head.T, preferred_element_type=jnp.float32)
        carry_out = (dk_sum + d_keys_part, dv_sum + d_values_part, dx_sum + dx_part)
        return carry_out, (dw_query_head, dw_out_head)

    carry_init = (jnp.zeros((SEQ_LEN, HEAD_DIM), jnp.float32), jnp.zeros((SEQ_LEN, HEAD_DIM), jnp.float32), jnp.zeros((SEQ_LEN, D_MODEL), jnp.float32))
    wq_heads = jnp.transpose(w_query, (1, 0, 2))
    sums_out, grads_out = lax.scan(head_step, carry_init, (wq_heads, w_out))
    dk_sum, dv_sum, dx_sum = sums_out
    dwq_heads, dw_out = grads_out
    d_keys = dk_sum.astype(jnp.bfloat16)
    d_values = dv_sum.astype(jnp.bfloat16)
    dw_key = jnp.dot(x_in.T, d_keys, preferred_element_type=jnp.float32)
    dw_value = jnp.dot(x_in.T, d_values, preferred_element_type=jnp.float32)
    dx_total = dx_sum + jnp.dot(d_keys, w_key.T, preferred_element_type=jnp.float32) + jnp.dot(d_values, w_value.T, preferred_element_type=jnp.float32)
    dx_out = dx_total.astype(jnp.bfloat16)
    dw_query = jnp.transpose(dwq_heads, (1, 0, 2))
    return (dx_out, dw_query, dw_key, dw_value, dw_out)
```

```python
import functools
import math
import jax
import jax.numpy as jnp
from jax import lax
from jax.experimental import pallas as pl
from jax.experimental.pallas import tpu as pltpu
from jax.sharding import PartitionSpec as P

MESH = pl.DeviceIdType.MESH
ANY = pl.BlockSpec(memory_space=pl.ANY)
VM = pl.BlockSpec(memory_space=pltpu.VMEM)
F32 = jnp.float32
BF = jnp.bfloat16
NT = (((1,), (1,)), ((), ()))
TN = (((0,), (0,)), ((), ()))

T, D, HL, E, R = 64, 6144, 12, 128, 16
NP = HL // 2
NC = 4
LEAD = 1
DC = D // NC
NX = 8
XC = D // NX
N1 = 512
N2 = 256


def attend_kernel(x_ref, dy_ref, wq_ref, wk_ref, wv_ref, wo_ref,
                  xt_ref, dyg_ref, ot_ref, dq_ref, dkv_ref, wkv, dxk_ref, dxs_ref,
                  xg, wq, wo, qacc, kvacc, doacc, dot_acc, q_s, o_s, do_s, dqp, part, keep, send, got,
                  lsem, wsem, link_s, link_r, pair_s, pair_r, fwd_s, fwd_r, ex_s, ex_r, red_s, red_r):
    scale = 1.0 / math.sqrt(E)
    m = lax.axis_index("model")
    core, chip = m % 2, m // 2
    partner = chip * 2 + (1 - core)
    counter = (1 - chip) * 2 + core
    diag = (1 - chip) * 2 + (1 - core)
    own = pl.ds(pl.multiple_of(m * R, R), R)
    far = pl.ds(pl.multiple_of(counter * R, R), R)
    bufs = (dyg_ref, xg)

    def cols(c):
        return pl.ds(c * DC, DC)

    loads = [pltpu.make_async_copy(s, g.at[own], lsem.at[a]) for a, (s, g) in enumerate(((dy_ref, dyg_ref), (x_ref, xg)))]
    for cp in loads:
        cp.start()
    wkv_cp = [pltpu.make_async_copy(s, wkv.at[:, pl.ds(j * E, E)], wsem.at[j]) for j, s in enumerate((wk_ref, wv_ref))]
    wq_cp = [[pltpu.make_async_copy(wq_ref.at[:, j, cols(c), :], wq.at[:, cols(c), pl.ds(j * E, E)], wsem.at[2 + 2 * c + j])
              for j in range(2)] for c in range(NC)]
    wo_cp = [pltpu.make_async_copy(wo_ref.at[:, cols(c)], wo.at[:, cols(c)], wsem.at[2 + 2 * NC + c]) for c in range(NC)]
    for cp in wo_cp[:NC // 2]:
        cp.start(priority=1)

    barrier = pltpu.get_barrier_semaphore()
    for peer in (partner, counter, diag):
        pl.semaphore_signal(barrier, inc=1, device_id={"model": peer}, device_id_type=MESH)
    pl.semaphore_wait(barrier, 3)

    link, pair, fwd = [], [], []
    for a in range(2):
        g = bufs[a]
        loads[a].wait()
        link.append([pltpu.make_async_remote_copy(g.at[own, cols(c)], g.at[own, cols(c)], link_s.at[a, c], link_r.at[a, c],
                                                  device_id={"model": counter}, device_id_type=MESH) for c in range(NC)])
        pair.append(pltpu.make_async_remote_copy(g.at[own], g.at[own], pair_s.at[a], pair_r.at[a],
                                                 device_id={"model": partner}, device_id_type=MESH))
        fwd.append([pltpu.make_async_remote_copy(g.at[far, cols(c)], g.at[far, cols(c)], fwd_s.at[a, c], fwd_r.at[a, c],
                                                 device_id={"model": partner}, device_id_type=MESH) for c in range(NC)])
        for cp in link[a]:
            cp.start()
        pair[a].start()

    for cp in wo_cp[NC // 2:] + wkv_cp:
        cp.start(priority=1)

    def relay(i):
        a, c = divmod(i, NC)
        if a < 2:
            link[a][c].wait_recv()
            fwd[a][c].start()

    for i in range(LEAD):
        relay(i)
    pair[0].wait_recv()
    for c in range(NC):
        relay(c + LEAD)
        fwd[0][c].wait_recv()
        wo_cp[c].wait()
        for cp in wq_cp[c]:
            cp.start(priority=1)
        dyc = dyg_ref[:, cols(c)]
        dyct = dyc.T
        for p in range(2):
            base = p * (N1 + N2)
            by_rows, by_cols = None, None
            for k in range(DC // 256):
                ks = pl.ds(c * DC + k * 256, 256)
                t1 = lax.dot_general(dyc[:, k * 256:(k + 1) * 256], wo[pl.ds(base, N1), ks], NT, preferred_element_type=F32)
                t2 = jnp.dot(wo[pl.ds(base + N1, N2), ks], dyct[k * 256:(k + 1) * 256, :], preferred_element_type=F32)
                by_rows = t1 if by_rows is None else by_rows + t1
                by_cols = t2 if by_cols is None else by_cols + t2
            if c == 0:
                doacc[p] = by_rows
                dot_acc[p] = by_cols
            else:
                doacc[p] += by_rows
                dot_acc[p] += by_cols
    for p in range(2):
        for j in range(6):
            rows = pl.ds((p * 6 + j) * T, T)
            if j < 4:
                do_s[rows, :] = doacc[p, :, j * E:(j + 1) * E].astype(BF)
            else:
                do_s[rows, :] = dot_acc[p, (j - 4) * E:(j - 3) * E, :].T.astype(BF)
    pair[1].wait_recv()
    for cp in wkv_cp:
        cp.wait()
    for c in range(NC):
        relay(NC + c + LEAD)
        fwd[1][c].wait_recv()
        for cp in wq_cp[c]:
            cp.wait()
        xc = xg[:, cols(c)]
        for p in range(NP):
            part_q = jnp.dot(xc, wq[p, cols(c), :], preferred_element_type=F32)
            if c == 0:
                qacc[p] = part_q
            else:
                qacc[p] += part_q
        part_kv = jnp.dot(xc, wkv[cols(c), :], preferred_element_type=F32)
        if c == 0:
            kvacc[...] = part_kv
        else:
            kvacc[...] += part_kv
        xt_ref[cols(c), :] = xc.T
    kv = kvacc[...].astype(BF)
    keys, vals = kv[:, :E], kv[:, E:]
    for p in range(NP):
        qp = qacc[p].astype(BF)
        q_s[pl.ds(2 * p * T, T), :] = qp[:, :E]
        q_s[pl.ds((2 * p + 1) * T, T), :] = qp[:, E:]
    d_attn = do_s[...]
    s = lax.dot_general(q_s[...], keys, NT, preferred_element_type=F32) * scale
    d_probs = lax.dot_general(d_attn, vals, NT, preferred_element_type=F32)
    row = lax.broadcasted_iota(jnp.int32, (HL * T, T), 0) % T
    col = lax.broadcasted_iota(jnp.int32, (HL * T, T), 1)
    s = jnp.where(row >= col, s, -jnp.inf)
    e = jnp.exp(s - jnp.max(s, axis=-1, keepdims=True))
    p32 = e / jnp.sum(e, axis=-1, keepdims=True)
    pb = p32.astype(BF)
    ob = jnp.dot(pb, vals, preferred_element_type=F32).astype(BF)
    o_s[...] = ob
    row_dot = jnp.sum(d_attn.astype(F32) * ob.astype(F32), axis=-1, keepdims=True)
    g = (p32 * (d_probs - row_dot) * scale).astype(BF)
    part[0, :, E:] = lax.dot_general(pb, d_attn, TN, preferred_element_type=F32)
    part[0, :, :E] = lax.dot_general(g, q_s[...], TN, preferred_element_type=F32)
    d_query = jnp.dot(g, keys, preferred_element_type=F32).astype(BF)
    for h in range(HL):
        dqh = d_query[h * T:(h + 1) * T, :]
        dq_ref[:, pl.ds(h * E, E)] = dqh
        for r in range(4):
            slot = (r // 2 + chip) % 2 * 2 + (r % 2 + core) % 2
            dqp[slot, :, pl.ds(h * E, E)] = dqh[r * R:(r + 1) * R, :]
    ex = [pltpu.make_async_remote_copy(part.at[2 * i], part.at[2 * i + 1], ex_s.at[i], ex_r.at[i], device_id={"model": peer}, device_id_type=MESH)
          for i, peer in enumerate((partner, counter))]
    ex[0].start()
    lhs = dqp[...].reshape(T, HL * E)
    red = [pltpu.make_async_remote_copy(send.at[:, :, pl.ds(c * XC, XC)], got.at[:, :, pl.ds(c * XC, XC)], red_s.at[c], red_r.at[c],
                                        device_id={"model": partner}, device_id_type=MESH) for c in range(NX)]

    lhst = lhs.T

    def dx_chunk(c):
        base = c * XC
        by_rows, by_cols = None, None
        for p in range(NP):
            ps = slice(p * 2 * E, (p + 1) * 2 * E)
            t1 = lax.dot_general(lhs[:, ps], wq[p, pl.ds(base, N1), :], NT, preferred_element_type=F32)
            t2 = jnp.dot(wq[p, pl.ds(base + N1, N2), :], lhst[ps, :], preferred_element_type=F32)
            by_rows = t1 if by_rows is None else by_rows + t1
            by_cols = t2 if by_cols is None else by_cols + t2
        by_cols = by_cols.T
        for k in range(4):
            dst, r = (send if k % 2 else keep), slice(k * R, (k + 1) * R)
            dst[k // 2, :, pl.ds(base, N1)] = by_rows[r, :]
            dst[k // 2, :, pl.ds(base + N1, N2)] = by_cols[r, :]

    def dx_sum(c):
        rows = pl.ds(c * XC, XC)
        red[c].wait_recv()
        dxk_ref[:, rows] = keep[0, :, rows] + got[0, :, rows]
        dxs_ref[:, rows] = keep[1, :, rows] + got[1, :, rows]

    for c in range(NX):
        dx_chunk(c)
        if c == 0:
            for h in range(HL):
                ot_ref[pl.ds(h * E, E), :] = o_s[pl.ds(h * T, T), :].T
        if c == 1:
            ex[0].wait_recv()
            part[2] = part[0] + part[1]
        if c == 2:
            ex[1].start()
        if c >= 1:
            red[c - 1].start()
    for c in range(NX - 2):
        dx_sum(c)
    red[NX - 1].start()
    dx_sum(NX - 2)
    ex[1].wait_recv()
    dkv_ref[...] = (part[2] + part[3]).astype(BF)
    dx_sum(NX - 1)
    for a in range(2):
        pair[a].wait_send()
        for c in range(NC):
            link[a][c].wait_send()
            fwd[a][c].wait_send()
    for cp in ex + red:
        cp.wait_send()


NB = 4
CW = D // 2
RQ = D // 4


def grads_kernel(xt_ref, dyg_ref, ot_ref, dq_ref, dkv_ref, wkv_ref, dx_ref, dwq_ref, dwo_ref, dwk_ref, dwv_ref, dxo_ref,
                 bo, bq, bkv, osem, qsem, ksem):
    m = lax.axis_index("model")

    def o_copy(i, j, slot):
        return pltpu.make_async_copy(bo.at[slot], dwo_ref.at[pl.ds(pl.multiple_of(i * E, E), E), pl.ds(j * CW, CW)], osem.at[slot])

    def q_copy(i, j, slot):
        rows = pl.ds(pl.multiple_of((i % 2) * (2 * RQ) + j * RQ, RQ), RQ)
        return pltpu.make_async_copy(bq.at[slot], dwq_ref.at[i // 2, :, rows, :], qsem.at[slot])

    def body(i, carry):
        ot = ot_ref[pl.ds(pl.multiple_of(i * E, E), E), :]
        dq = dq_ref[:, pl.ds(pl.multiple_of((i // 2) * 2 * E, 2 * E), 2 * E)]
        for j in range(2):
            slot = (i % 2) * 2 + j

            @pl.when(i >= 2)
            def _():
                o_copy(i - 2, j, slot).wait()

            bo[slot] = jnp.dot(ot, dyg_ref[:, j * CW:(j + 1) * CW], preferred_element_type=F32)
            o_copy(i, j, slot).start()

            @pl.when(i >= 2)
            def _():
                q_copy(i - 2, j, slot).wait()

            rows = pl.ds(pl.multiple_of((i % 2) * (2 * RQ) + j * RQ, RQ), RQ)
            v = jnp.dot(xt_ref[rows, :], dq, preferred_element_type=F32)
            bq[slot, 0] = v[:, :E]
            bq[slot, 1] = v[:, E:]
            q_copy(i, j, slot).start()
        return carry

    lax.fori_loop(0, HL, body, 0)
    v = jnp.dot(xt_ref[pl.ds(pl.multiple_of(m * RQ, RQ), RQ), :], dkv_ref[...], preferred_element_type=F32)
    bkv[0] = v[:, :E]
    bkv[1] = v[:, E:]
    k_cp = [pltpu.make_async_copy(bkv.at[j], r, ksem.at[j]) for j, r in enumerate((dwk_ref, dwv_ref))]
    for cp in k_cp:
        cp.start()
    mine = dkv_ref[pl.ds(pl.multiple_of(m * R, R), R), :]
    dxo_ref[...] = dx_ref[...] + lax.dot_general(mine, wkv_ref[...], NT, preferred_element_type=F32)
    for i in (HL - 2, HL - 1):
        for j in range(2):
            o_copy(i, j, (i % 2) * 2 + j).wait()
            q_copy(i, j, (i % 2) * 2 + j).wait()
    for cp in k_cp:
        cp.wait()


def solution(mesh):
    tok = P(("data", "model"), None)

    def step(x, dy, w_query, w_key, w_value, w_out):
        wq = jnp.transpose(w_query, (1, 0, 2)).reshape(NP, 2, D, E)
        wo = w_out.reshape(HL * E, D)
        S = jax.ShapeDtypeStruct
        DMA = pltpu.SemaphoreType.DMA
        V = pltpu.VMEM
        xt, dyg, ot, dq, dkv, wkv, dxk, dxs = pl.pallas_call(
            attend_kernel,
            out_shape=[V((D, T), BF), V((T, D), BF), V((HL * E, T), BF), V((T, HL * E), BF), V((T, 2 * E), BF), V((D, 2 * E), BF), V((R, D), F32), S((R, D), F32)],
            in_specs=[ANY] * 6,
            out_specs=[VM] * 8,
            scratch_shapes=[
                V((T, D), BF), V((NP, D, 2 * E), BF), V((HL * E, D), BF), V((NP, T, 2 * E), F32), V((T, 2 * E), F32),
                V((2, T, N1), F32), V((2, N2, T), F32), V((HL * T, E), BF), V((HL * T, E), BF), V((HL * T, E), BF),
                V((4, R, HL * E), BF), V((4, T, 2 * E), F32), V((2, R, D), F32), V((2, R, D), F32), V((2, R, D), F32),
                DMA((2,)), DMA((2 + 3 * NC,)), DMA((2, NC)), DMA((2, NC)), DMA((2,)), DMA((2,)), DMA((2, NC)), DMA((2, NC)),
                DMA((2,)), DMA((2,)), DMA((NX,)), DMA((NX,)),
            ],
            compiler_params=pltpu.CompilerParams(collective_id=0, has_side_effects=True, vmem_limit_bytes=50 * 2**20),
            cost_estimate=pl.CostEstimate(flops=10**10, bytes_accessed=4 * 10**7, transcendentals=0),
            name="attend",
        )(x, dy, wq, w_key, w_value, wo)
        far = lax.ppermute(dxs, "model", [(0, 2), (2, 0), (1, 3), (3, 1)])
        dwq, dwo, dwk, dwv, dxo = pl.pallas_call(
            grads_kernel,
            out_shape=[S((NP, 2, D, E), F32), S((HL * E, D), F32), S((RQ, E), F32), S((RQ, E), F32), S((R, D), F32)],
            in_specs=[VM] * 7,
            out_specs=[ANY] * 4 + [VM],
            scratch_shapes=[V((NB, E, CW), F32), V((NB, 2, RQ, E), F32), V((2, RQ, E), F32), DMA((NB,)), DMA((NB,)), DMA((2,))],
            compiler_params=pltpu.CompilerParams(vmem_limit_bytes=24 * 2**20),
            cost_estimate=pl.CostEstimate(flops=4 * 10**10, bytes_accessed=8 * 10**7, transcendentals=0),
            name="grads",
        )(xt, dyg, ot, dq, dkv, wkv, dxk)
        dx = (dxo + far).astype(BF)
        dw_query = jnp.transpose(dwq.reshape(HL, D, E), (1, 0, 2))
        return dx, dw_query, dwk, dwv, dwo.reshape(HL, E, D)

    return jax.shard_map(step, mesh=mesh, in_specs=(tok, tok, P(None, "model", None), P(None, None), P(None, None), P("model", None, None)),
                         out_specs=(tok, P("data", "model", None), tok, tok, P(("data", "model"), None, None)), check_vma=False)
```

```python
import functools
import math
import jax
import jax.numpy as jnp
from jax import lax
from jax.experimental import pallas as pl
from jax.experimental.pallas import tpu as pltpu
from jax.sharding import PartitionSpec as P

MESH = pl.DeviceIdType.MESH
ANY = pl.BlockSpec(memory_space=pl.ANY)
VM = pl.BlockSpec(memory_space=pltpu.VMEM)
F32 = jnp.float32
BF = jnp.bfloat16
NT = (((1,), (1,)), ((), ()))
TN = (((0,), (0,)), ((), ()))

T, D, HL, E, R = 64, 6144, 12, 128, 16
NP = HL // 2
LEAD = 1
SIZES = ((1536, 1536, 1536, 1536), (2048, 2048, 1536, 512))
STARTS = tuple(tuple(sum(sz[:c]) for c in range(len(sz))) for sz in SIZES)
NY, NQ = len(SIZES[0]), len(SIZES[1])
NC = max(NY, NQ)
N1 = 512
N2 = 256
XB = N1 + N2
XS = (3, 3, 2)
NX = len(XS)
X0 = tuple(sum(XS[:c]) for c in range(NX))


def attend_kernel(x_ref, dy_ref, wq_ref, wk_ref, wv_ref, wo_ref,
                  xt_ref, dyg_ref, ot_ref, dq_ref, dkv_ref, wkv, dxk_ref, dxs_ref,
                  xg, wq, wo, qacc, kvacc, doacc, dot_acc, q_s, o_s, do_s, dqp, part, keep, send, got,
                  lsem, wsem, link_s, link_r, pair_s, pair_r, fwd_s, fwd_r, ex_s, ex_r, red_s, red_r):
    scale = 1.0 / math.sqrt(E)
    m = lax.axis_index("model")
    core, chip = m % 2, m // 2
    partner = chip * 2 + (1 - core)
    counter = (1 - chip) * 2 + core
    diag = (1 - chip) * 2 + (1 - core)
    own = pl.ds(pl.multiple_of(m * R, R), R)
    far = pl.ds(pl.multiple_of(counter * R, R), R)
    bufs = (dyg_ref, xg)

    def cols(a, c):
        return pl.ds(STARTS[a][c], SIZES[a][c])

    loads = [pltpu.make_async_copy(s, g.at[own], lsem.at[a]) for a, (s, g) in enumerate(((dy_ref, dyg_ref), (x_ref, xg)))]
    for cp in loads:
        cp.start()
    wkv_cp = [pltpu.make_async_copy(s, wkv.at[:, pl.ds(j * E, E)], wsem.at[j]) for j, s in enumerate((wk_ref, wv_ref))]
    wq_cp = [[pltpu.make_async_copy(wq_ref.at[:, j, cols(1, c), :], wq.at[:, cols(1, c), pl.ds(j * E, E)], wsem.at[2 + 2 * c + j])
              for j in range(2)] for c in range(NQ)]
    wo_cp = [pltpu.make_async_copy(wo_ref.at[:, cols(0, c)], wo.at[:, cols(0, c)], wsem.at[2 + 2 * NQ + c]) for c in range(NY)]
    for cp in wo_cp[:NY // 2]:
        cp.start(priority=1)

    barrier = pltpu.get_barrier_semaphore()
    for peer in (partner, counter, diag):
        pl.semaphore_signal(barrier, inc=1, device_id={"model": peer}, device_id_type=MESH)
    pl.semaphore_wait(barrier, 3)

    link, pair, fwd = [], [], []
    for a in range(2):
        g = bufs[a]
        loads[a].wait()
        link.append([pltpu.make_async_remote_copy(g.at[own, cols(a, c)], g.at[own, cols(a, c)], link_s.at[a, c], link_r.at[a, c],
                                                  device_id={"model": counter}, device_id_type=MESH) for c in range(len(SIZES[a]))])
        pair.append(pltpu.make_async_remote_copy(g.at[own], g.at[own], pair_s.at[a], pair_r.at[a],
                                                 device_id={"model": partner}, device_id_type=MESH))
        fwd.append([pltpu.make_async_remote_copy(g.at[far, cols(a, c)], g.at[far, cols(a, c)], fwd_s.at[a, c], fwd_r.at[a, c],
                                                 device_id={"model": partner}, device_id_type=MESH) for c in range(len(SIZES[a]))])
        for cp in link[a]:
            cp.start()
        pair[a].start()

    for cp in wo_cp[NY // 2:] + wkv_cp:
        cp.start(priority=1)

    def relay(i):
        a, c = (0, i) if i < NY else (1, i - NY)
        if c < len(SIZES[a]):
            link[a][c].wait_recv()
            fwd[a][c].start()

    for i in range(LEAD):
        relay(i)
    pair[0].wait_recv()
    for c in range(NY):
        relay(c + LEAD)
        fwd[0][c].wait_recv()
        wo_cp[c].wait()
        for cp in wq_cp[c] + (sum(wq_cp[NY:], []) if c == NY - 1 else []):
            cp.start(priority=1)
        dyc = dyg_ref[:, cols(0, c)]
        dyct = dyc.T
        for p in range(2):
            base = p * (N1 + N2)
            by_rows, by_cols = None, None
            for k in range(SIZES[0][c] // 256):
                ks = pl.ds(STARTS[0][c] + k * 256, 256)
                t1 = lax.dot_general(dyc[:, k * 256:(k + 1) * 256], wo[pl.ds(base, N1), ks], NT, preferred_element_type=F32)
                t2 = jnp.dot(wo[pl.ds(base + N1, N2), ks], dyct[k * 256:(k + 1) * 256, :], preferred_element_type=F32)
                by_rows = t1 if by_rows is None else by_rows + t1
                by_cols = t2 if by_cols is None else by_cols + t2
            if c == 0:
                doacc[p] = by_rows
                dot_acc[p] = by_cols
            else:
                doacc[p] += by_rows
                dot_acc[p] += by_cols
    for p in range(2):
        for j in range(6):
            rows = pl.ds((p * 6 + j) * T, T)
            if j < 4:
                do_s[rows, :] = doacc[p, :, j * E:(j + 1) * E].astype(BF)
            else:
                do_s[rows, :] = dot_acc[p, (j - 4) * E:(j - 3) * E, :].T.astype(BF)
    pair[1].wait_recv()
    for cp in wkv_cp:
        cp.wait()
    for c in range(NQ):
        relay(NY + c + LEAD)
        fwd[1][c].wait_recv()
        for cp in wq_cp[c]:
            cp.wait()
        xc = xg[:, cols(1, c)]
        for p in range(NP):
            part_q = jnp.dot(xc, wq[p, cols(1, c), :], preferred_element_type=F32)
            if c == 0:
                qacc[p] = part_q
            else:
                qacc[p] += part_q
        part_kv = jnp.dot(xc, wkv[cols(1, c), :], preferred_element_type=F32)
        if c == 0:
            kvacc[...] = part_kv
        else:
            kvacc[...] += part_kv
        xt_ref[cols(1, c), :] = xc.T
    kv = kvacc[...].astype(BF)
    keys, vals = kv[:, :E], kv[:, E:]
    for p in range(NP):
        qp = qacc[p].astype(BF)
        q_s[pl.ds(2 * p * T, T), :] = qp[:, :E]
        q_s[pl.ds((2 * p + 1) * T, T), :] = qp[:, E:]
    d_attn = do_s[...]
    s = lax.dot_general(q_s[...], keys, NT, preferred_element_type=F32) * scale
    d_probs = lax.dot_general(d_attn, vals, NT, preferred_element_type=F32)
    row = lax.broadcasted_iota(jnp.int32, (HL * T, T), 0) % T
    col = lax.broadcasted_iota(jnp.int32, (HL * T, T), 1)
    s = jnp.where(row >= col, s, -jnp.inf)
    e = jnp.exp(s - jnp.max(s, axis=-1, keepdims=True))
    p32 = e / jnp.sum(e, axis=-1, keepdims=True)
    pb = p32.astype(BF)
    ob = jnp.dot(pb, vals, preferred_element_type=F32).astype(BF)
    o_s[...] = ob
    row_dot = jnp.sum(d_attn.astype(F32) * ob.astype(F32), axis=-1, keepdims=True)
    g = (p32 * (d_probs - row_dot) * scale).astype(BF)
    part[0, :, E:] = lax.dot_general(pb, d_attn, TN, preferred_element_type=F32)
    part[0, :, :E] = lax.dot_general(g, q_s[...], TN, preferred_element_type=F32)
    d_query = jnp.dot(g, keys, preferred_element_type=F32).astype(BF)
    for h in range(HL):
        dqh = d_query[h * T:(h + 1) * T, :]
        dq_ref[:, pl.ds(h * E, E)] = dqh
        for r in range(4):
            slot = (r // 2 + chip) % 2 * 2 + (r % 2 + core) % 2
            dqp[slot, :, pl.ds(h * E, E)] = dqh[r * R:(r + 1) * R, :]
    ex = [pltpu.make_async_remote_copy(part.at[0], part.at[i + 1], ex_s.at[i], ex_r.at[i], device_id={"model": peer}, device_id_type=MESH)
          for i, peer in enumerate((partner, counter, diag))]
    for cp in ex:
        cp.start()
    lhs = dqp[...].reshape(T, HL * E)
    def xcols(c):
        return pl.ds(X0[c] * XB, XS[c] * XB)

    red = [pltpu.make_async_remote_copy(send.at[:, :, xcols(c)], got.at[:, :, xcols(c)], red_s.at[c], red_r.at[c],
                                        device_id={"model": partner}, device_id_type=MESH) for c in range(NX)]

    lhst = lhs.T

    def dx_block(base):
        by_rows, by_cols = None, None
        for p in range(NP):
            ps = slice(p * 2 * E, (p + 1) * 2 * E)
            t1 = lax.dot_general(lhs[:, ps], wq[p, pl.ds(base, N1), :], NT, preferred_element_type=F32)
            t2 = jnp.dot(wq[p, pl.ds(base + N1, N2), :], lhst[ps, :], preferred_element_type=F32)
            by_rows = t1 if by_rows is None else by_rows + t1
            by_cols = t2 if by_cols is None else by_cols + t2
        by_cols = by_cols.T
        for k in range(4):
            dst, r = (send if k % 2 else keep), slice(k * R, (k + 1) * R)
            dst[k // 2, :, pl.ds(base, N1)] = by_rows[r, :]
            dst[k // 2, :, pl.ds(base + N1, N2)] = by_cols[r, :]

    def dx_sum(c):
        rows = xcols(c)
        red[c].wait_recv()
        dxk_ref[:, rows] = keep[0, :, rows] + got[0, :, rows]
        dxs_ref[:, rows] = keep[1, :, rows] + got[1, :, rows]

    for c in range(NX):
        for i in range(XS[c]):
            dx_block((X0[c] + i) * XB)
        if c >= 1:
            red[c - 1].start()
    for h in range(HL):
        ot_ref[pl.ds(h * E, E), :] = o_s[pl.ds(h * T, T), :].T
    red[NX - 1].start()
    for c in range(NX - 1):
        dx_sum(c)
    for cp in ex:
        cp.wait_recv()
    dkv_ref[...] = ((part[0] + part[1]) + (part[2] + part[3])).astype(BF)
    dx_sum(NX - 1)
    for a in range(2):
        pair[a].wait_send()
        for cp in link[a] + fwd[a]:
            cp.wait_send()
    for cp in ex + red:
        cp.wait_send()


NB = 4
CW = D // 2
RQ = D // 4


def grads_kernel(xt_ref, dyg_ref, ot_ref, dq_ref, dkv_ref, wkv_ref, dx_ref, dwq_ref, dwo_ref, dwk_ref, dwv_ref, dxo_ref,
                 bo, bq, bkv, osem, qsem, ksem):
    m = lax.axis_index("model")

    def o_copy(i, j, slot):
        return pltpu.make_async_copy(bo.at[slot], dwo_ref.at[pl.ds(pl.multiple_of(i * E, E), E), pl.ds(j * CW, CW)], osem.at[slot])

    def q_copy(i, j, slot):
        rows = pl.ds(pl.multiple_of((i % 2) * (2 * RQ) + j * RQ, RQ), RQ)
        return pltpu.make_async_copy(bq.at[slot], dwq_ref.at[i // 2, :, rows, :], qsem.at[slot])

    def body(i, carry):
        ot = ot_ref[pl.ds(pl.multiple_of(i * E, E), E), :]
        dq = dq_ref[:, pl.ds(pl.multiple_of((i // 2) * 2 * E, 2 * E), 2 * E)]
        for j in range(2):
            slot = (i % 2) * 2 + j

            @pl.when(i >= 2)
            def _():
                o_copy(i - 2, j, slot).wait()

            bo[slot] = jnp.dot(ot, dyg_ref[:, j * CW:(j + 1) * CW], preferred_element_type=F32)
            o_copy(i, j, slot).start()

            @pl.when(i >= 2)
            def _():
                q_copy(i - 2, j, slot).wait()

            rows = pl.ds(pl.multiple_of((i % 2) * (2 * RQ) + j * RQ, RQ), RQ)
            v = jnp.dot(xt_ref[rows, :], dq, preferred_element_type=F32)
            bq[slot, 0] = v[:, :E]
            bq[slot, 1] = v[:, E:]
            q_copy(i, j, slot).start()
        return carry

    lax.fori_loop(0, HL, body, 0)
    v = jnp.dot(xt_ref[pl.ds(pl.multiple_of(m * RQ, RQ), RQ), :], dkv_ref[...], preferred_element_type=F32)
    bkv[0] = v[:, :E]
    bkv[1] = v[:, E:]
    k_cp = [pltpu.make_async_copy(bkv.at[j], r, ksem.at[j]) for j, r in enumerate((dwk_ref, dwv_ref))]
    for cp in k_cp:
        cp.start()
    mine = dkv_ref[pl.ds(pl.multiple_of(m * R, R), R), :]
    dxo_ref[...] = dx_ref[...] + lax.dot_general(mine, wkv_ref[...], NT, preferred_element_type=F32)
    for i in (HL - 2, HL - 1):
        for j in range(2):
            o_copy(i, j, (i % 2) * 2 + j).wait()
            q_copy(i, j, (i % 2) * 2 + j).wait()
    for cp in k_cp:
        cp.wait()


def solution(mesh):
    tok = P(("data", "model"), None)

    def step(x, dy, w_query, w_key, w_value, w_out):
        wq = jnp.transpose(w_query, (1, 0, 2)).reshape(NP, 2, D, E)
        wo = w_out.reshape(HL * E, D)
        S = jax.ShapeDtypeStruct
        DMA = pltpu.SemaphoreType.DMA
        V = pltpu.VMEM
        xt, dyg, ot, dq, dkv, wkv, dxk, dxs = pl.pallas_call(
            attend_kernel,
            out_shape=[V((D, T), BF), V((T, D), BF), V((HL * E, T), BF), V((T, HL * E), BF), V((T, 2 * E), BF), V((D, 2 * E), BF), V((R, D), F32), V((R, D), F32)],
            in_specs=[ANY] * 6,
            out_specs=[VM] * 8,
            scratch_shapes=[
                V((T, D), BF), V((NP, D, 2 * E), BF), V((HL * E, D), BF), V((NP, T, 2 * E), F32), V((T, 2 * E), F32),
                V((2, T, N1), F32), V((2, N2, T), F32), V((HL * T, E), BF), V((HL * T, E), BF), V((HL * T, E), BF),
                V((4, R, HL * E), BF), V((4, T, 2 * E), F32), V((2, R, D), F32), V((2, R, D), F32), V((2, R, D), F32),
                DMA((2,)), DMA((2 + 2 * NQ + NY,)), DMA((2, NC)), DMA((2, NC)), DMA((2,)), DMA((2,)), DMA((2, NC)), DMA((2, NC)),
                DMA((3,)), DMA((3,)), DMA((NX,)), DMA((NX,)),
            ],
            compiler_params=pltpu.CompilerParams(collective_id=0, has_side_effects=True, vmem_limit_bytes=50 * 2**20),
            cost_estimate=pl.CostEstimate(flops=10**10, bytes_accessed=4 * 10**7, transcendentals=0),
            name="attend",
        )(x, dy, wq, w_key, w_value, wo)
        far = lax.ppermute(dxs, "model", [(0, 2), (2, 0), (1, 3), (3, 1)])
        dwq, dwo, dwk, dwv, dxo = pl.pallas_call(
            grads_kernel,
            out_shape=[S((NP, 2, D, E), F32), S((HL * E, D), F32), S((RQ, E), F32), S((RQ, E), F32), S((R, D), F32)],
            in_specs=[VM] * 7,
            out_specs=[ANY] * 4 + [VM],
            scratch_shapes=[V((NB, E, CW), F32), V((NB, 2, RQ, E), F32), V((2, RQ, E), F32), DMA((NB,)), DMA((NB,)), DMA((2,))],
            compiler_params=pltpu.CompilerParams(vmem_limit_bytes=24 * 2**20),
            cost_estimate=pl.CostEstimate(flops=4 * 10**10, bytes_accessed=8 * 10**7, transcendentals=0),
            name="grads",
        )(xt, dyg, ot, dq, dkv, wkv, dxk)
        dx = (dxo + far).astype(BF)
        dw_query = jnp.transpose(dwq.reshape(HL, D, E), (1, 0, 2))
        return dx, dw_query, dwk, dwv, dwo.reshape(HL, E, D)

    return jax.shard_map(step, mesh=mesh, in_specs=(tok, tok, P(None, "model", None), P(None, None), P(None, None), P("model", None, None)),
                         out_specs=(tok, P("data", "model", None), tok, tok, P(("data", "model"), None, None)), check_vma=False)
```

```python
import functools
import math
import jax
import jax.numpy as jnp
from jax import lax
from jax.experimental import pallas as pl
from jax.experimental.pallas import tpu as pltpu
from jax.sharding import PartitionSpec as P

MESH = pl.DeviceIdType.MESH
ANY = pl.BlockSpec(memory_space=pl.ANY)
VM = pl.BlockSpec(memory_space=pltpu.VMEM)
F32 = jnp.float32
BF = jnp.bfloat16
NT = (((1,), (1,)), ((), ()))
TN = (((0,), (0,)), ((), ()))

T, D, HL, E, R = 64, 6144, 12, 128, 16
NP = HL // 2
LEAD = 1
SIZES = ((1536, 1536, 1536, 1536), (2048, 2048, 1536, 512))
STARTS = tuple(tuple(sum(sz[:c]) for c in range(len(sz))) for sz in SIZES)
NY, NQ = len(SIZES[0]), len(SIZES[1])
NC = max(NY, NQ)
N1 = 512
N2 = 256
XB = N1 + N2
XS = (3, 3, 2)
NX = len(XS)
X0 = tuple(sum(XS[:c]) for c in range(NX))


def attend_kernel(x_ref, dy_ref, wq_ref, wk_ref, wv_ref, wo_ref,
                  xt_ref, dyg_ref, ot_ref, dq_ref, dkv_ref, wkv, dxk_ref, dxs_ref,
                  xg, wq, wo, qacc, kvacc, doacc, dot_acc, q_s, o_s, do_s, dqp, part, keep, send, got,
                  lsem, wsem, link_s, link_r, pair_s, pair_r, fwd_s, fwd_r, ex_s, ex_r, red_s, red_r):
    scale = 1.0 / math.sqrt(E)
    m = lax.axis_index("model")
    core, chip = m % 2, m // 2
    partner = chip * 2 + (1 - core)
    counter = (1 - chip) * 2 + core
    diag = (1 - chip) * 2 + (1 - core)
    own = pl.ds(pl.multiple_of(m * R, R), R)
    far = pl.ds(pl.multiple_of(counter * R, R), R)
    bufs = (dyg_ref, xg)

    def cols(a, c):
        return pl.ds(STARTS[a][c], SIZES[a][c])

    loads = [pltpu.make_async_copy(s, g.at[own], lsem.at[a]) for a, (s, g) in enumerate(((dy_ref, dyg_ref), (x_ref, xg)))]
    for cp in loads:
        cp.start()
    wkv_cp = [pltpu.make_async_copy(s, wkv.at[:, pl.ds(j * E, E)], wsem.at[j]) for j, s in enumerate((wk_ref, wv_ref))]
    wq_cp = [[pltpu.make_async_copy(wq_ref.at[:, j, cols(1, c), :], wq.at[:, cols(1, c), pl.ds(j * E, E)], wsem.at[2 + 2 * c + j])
              for j in range(2)] for c in range(NQ)]
    wo_cp = [pltpu.make_async_copy(wo_ref.at[:, cols(0, c)], wo.at[:, cols(0, c)], wsem.at[2 + 2 * NQ + c]) for c in range(NY)]
    for cp in wo_cp[:NY // 2]:
        cp.start(priority=1)

    barrier = pltpu.get_barrier_semaphore()
    for peer in (partner, counter, diag):
        pl.semaphore_signal(barrier, inc=1, device_id={"model": peer}, device_id_type=MESH)
    pl.semaphore_wait(barrier, 3)

    link, pair, fwd = [], [], []
    for a in range(2):
        g = bufs[a]
        loads[a].wait()
        link.append([pltpu.make_async_remote_copy(g.at[own, cols(a, c)], g.at[own, cols(a, c)], link_s.at[a, c], link_r.at[a, c],
                                                  device_id={"model": counter}, device_id_type=MESH) for c in range(len(SIZES[a]))])
        pair.append(pltpu.make_async_remote_copy(g.at[own], g.at[own], pair_s.at[a], pair_r.at[a],
                                                 device_id={"model": partner}, device_id_type=MESH))
        fwd.append([pltpu.make_async_remote_copy(g.at[far, cols(a, c)], g.at[far, cols(a, c)], fwd_s.at[a, c], fwd_r.at[a, c],
                                                 device_id={"model": partner}, device_id_type=MESH) for c in range(len(SIZES[a]))])
        for cp in link[a]:
            cp.start()
        pair[a].start()

    for cp in wo_cp[NY // 2:] + wkv_cp:
        cp.start(priority=1)

    def relay(i):
        a, c = (0, i) if i < NY else (1, i - NY)
        if c < len(SIZES[a]):
            link[a][c].wait_recv()
            fwd[a][c].start()

    for i in range(LEAD):
        relay(i)
    pair[0].wait_recv()
    for c in range(NY):
        relay(c + LEAD)
        fwd[0][c].wait_recv()
        wo_cp[c].wait()
        for cp in wq_cp[c] + (sum(wq_cp[NY:], []) if c == NY - 1 else []):
            cp.start(priority=1)
        dyc = dyg_ref[:, cols(0, c)]
        dyct = dyc.T
        for p in range(2):
            base = p * (N1 + N2)
            by_rows, by_cols = None, None
            for k in range(SIZES[0][c] // 256):
                ks = pl.ds(STARTS[0][c] + k * 256, 256)
                t1 = lax.dot_general(dyc[:, k * 256:(k + 1) * 256], wo[pl.ds(base, N1), ks], NT, preferred_element_type=F32)
                t2 = jnp.dot(wo[pl.ds(base + N1, N2), ks], dyct[k * 256:(k + 1) * 256, :], preferred_element_type=F32)
                by_rows = t1 if by_rows is None else by_rows + t1
                by_cols = t2 if by_cols is None else by_cols + t2
            if c == 0:
                doacc[p] = by_rows
                dot_acc[p] = by_cols
            else:
                doacc[p] += by_rows
                dot_acc[p] += by_cols
    for p in range(2):
        for j in range(6):
            rows = pl.ds((p * 6 + j) * T, T)
            if j < 4:
                do_s[rows, :] = doacc[p, :, j * E:(j + 1) * E].astype(BF)
            else:
                do_s[rows, :] = dot_acc[p, (j - 4) * E:(j - 3) * E, :].T.astype(BF)
    pair[1].wait_recv()
    for cp in wkv_cp:
        cp.wait()
    for c in range(NQ):
        relay(NY + c + LEAD)
        fwd[1][c].wait_recv()
        for cp in wq_cp[c]:
            cp.wait()
        xc = xg[:, cols(1, c)]
        for p in range(NP):
            part_q = jnp.dot(xc, wq[p, cols(1, c), :], preferred_element_type=F32)
            if c == 0:
                qacc[p] = part_q
            else:
                qacc[p] += part_q
        part_kv = jnp.dot(xc, wkv[cols(1, c), :], preferred_element_type=F32)
        if c == 0:
            kvacc[...] = part_kv
        else:
            kvacc[...] += part_kv
        xt_ref[cols(1, c), :] = xc.T
    kv = kvacc[...].astype(BF)
    keys, vals = kv[:, :E], kv[:, E:]
    for p in range(NP):
        qp = qacc[p].astype(BF)
        q_s[pl.ds(2 * p * T, T), :] = qp[:, :E]
        q_s[pl.ds((2 * p + 1) * T, T), :] = qp[:, E:]
    d_attn = do_s[...]
    s = lax.dot_general(q_s[...], keys, NT, preferred_element_type=F32) * scale
    d_probs = lax.dot_general(d_attn, vals, NT, preferred_element_type=F32)
    row = lax.broadcasted_iota(jnp.int32, (HL * T, T), 0) % T
    col = lax.broadcasted_iota(jnp.int32, (HL * T, T), 1)
    s = jnp.where(row >= col, s, -jnp.inf)
    e = jnp.exp(s - jnp.max(s, axis=-1, keepdims=True))
    p32 = e / jnp.sum(e, axis=-1, keepdims=True)
    pb = p32.astype(BF)
    ob = jnp.dot(pb, vals, preferred_element_type=F32).astype(BF)
    o_s[...] = ob
    row_dot = jnp.sum(d_attn.astype(F32) * ob.astype(F32), axis=-1, keepdims=True)
    g = (p32 * (d_probs - row_dot) * scale).astype(BF)
    part[0, :, E:] = lax.dot_general(pb, d_attn, TN, preferred_element_type=F32)
    part[0, :, :E] = lax.dot_general(g, q_s[...], TN, preferred_element_type=F32)
    d_query = jnp.dot(g, keys, preferred_element_type=F32).astype(BF)
    for h in range(HL):
        dqh = d_query[h * T:(h + 1) * T, :]
        dq_ref[:, pl.ds(h * E, E)] = dqh
        for r in range(4):
            slot = (r // 2 + chip) % 2 * 2 + (r % 2 + core) % 2
            dqp[slot, :, pl.ds(h * E, E)] = dqh[r * R:(r + 1) * R, :]
    ex = [pltpu.make_async_remote_copy(part.at[0], part.at[i + 1], ex_s.at[i], ex_r.at[i], device_id={"model": peer}, device_id_type=MESH)
          for i, peer in enumerate((partner, counter, diag))]
    for cp in ex:
        cp.start()
    lhs = dqp[...].reshape(T, HL * E)
    def xcols(c):
        return pl.ds(X0[c] * XB, XS[c] * XB)

    red = [pltpu.make_async_remote_copy(send.at[:, :, xcols(c)], got.at[:, :, xcols(c)], red_s.at[c], red_r.at[c],
                                        device_id={"model": partner}, device_id_type=MESH) for c in range(NX)]


    def dx_block(base):
        by_rows, by_cols = None, None
        for p in range(NP):
            ps = slice(p * 2 * E, (p + 1) * 2 * E)
            t1 = lax.dot_general(lhs[:, ps], wq[p, pl.ds(base, N1), :], NT, preferred_element_type=F32)
            t2 = lax.dot_general(wq[p, pl.ds(base + N1, N2), :], lhs[:, ps], NT, preferred_element_type=F32)
            by_rows = t1 if by_rows is None else by_rows + t1
            by_cols = t2 if by_cols is None else by_cols + t2
        by_cols = by_cols.T
        for k in range(4):
            dst, r = (send if k % 2 else keep), slice(k * R, (k + 1) * R)
            dst[k // 2, :, pl.ds(base, N1)] = by_rows[r, :]
            dst[k // 2, :, pl.ds(base + N1, N2)] = by_cols[r, :]

    def dx_sum(c):
        rows = xcols(c)
        red[c].wait_recv()
        dxk_ref[:, rows] = keep[0, :, rows] + got[0, :, rows]
        dxs_ref[:, rows] = keep[1, :, rows] + got[1, :, rows]

    for c in range(NX):
        for i in range(XS[c]):
            dx_block((X0[c] + i) * XB)
        if c >= 1:
            red[c - 1].start()
    for h in range(HL):
        ot_ref[pl.ds(h * E, E), :] = o_s[pl.ds(h * T, T), :].T
    red[NX - 1].start()
    for c in range(NX - 1):
        dx_sum(c)
    for cp in ex:
        cp.wait_recv()
    dkv_ref[...] = ((part[0] + part[1]) + (part[2] + part[3])).astype(BF)
    dx_sum(NX - 1)
    for a in range(2):
        pair[a].wait_send()
        for cp in link[a] + fwd[a]:
            cp.wait_send()
    for cp in ex + red:
        cp.wait_send()


NB = 4
CW = D // 2
RQ = D // 4


def grads_kernel(xt_ref, dyg_ref, ot_ref, dq_ref, dkv_ref, wkv_ref, dx_ref, dwq_ref, dwo_ref, dwk_ref, dwv_ref, dxo_ref,
                 bo, bq, bkv, osem, qsem, ksem):
    m = lax.axis_index("model")

    def o_copy(i, j, slot):
        return pltpu.make_async_copy(bo.at[slot], dwo_ref.at[pl.ds(pl.multiple_of(i * E, E), E), pl.ds(j * CW, CW)], osem.at[slot])

    def q_copy(i, j, slot):
        rows = pl.ds(pl.multiple_of((i % 2) * (2 * RQ) + j * RQ, RQ), RQ)
        return pltpu.make_async_copy(bq.at[slot], dwq_ref.at[i // 2, :, rows, :], qsem.at[slot])

    def body(i, carry):
        ot = ot_ref[pl.ds(pl.multiple_of(i * E, E), E), :]
        dq = dq_ref[:, pl.ds(pl.multiple_of((i // 2) * 2 * E, 2 * E), 2 * E)]
        for j in range(2):
            slot = (i % 2) * 2 + j

            @pl.when(i >= 2)
            def _():
                o_copy(i - 2, j, slot).wait()

            bo[slot] = jnp.dot(ot, dyg_ref[:, j * CW:(j + 1) * CW], preferred_element_type=F32)
            o_copy(i, j, slot).start()

            @pl.when(i >= 2)
            def _():
                q_copy(i - 2, j, slot).wait()

            rows = pl.ds(pl.multiple_of((i % 2) * (2 * RQ) + j * RQ, RQ), RQ)
            v = jnp.dot(xt_ref[rows, :], dq, preferred_element_type=F32)
            bq[slot, 0] = v[:, :E]
            bq[slot, 1] = v[:, E:]
            q_copy(i, j, slot).start()
        return carry

    lax.fori_loop(0, HL, body, 0)
    v = jnp.dot(xt_ref[pl.ds(pl.multiple_of(m * RQ, RQ), RQ), :], dkv_ref[...], preferred_element_type=F32)
    bkv[0] = v[:, :E]
    bkv[1] = v[:, E:]
    k_cp = [pltpu.make_async_copy(bkv.at[j], r, ksem.at[j]) for j, r in enumerate((dwk_ref, dwv_ref))]
    for cp in k_cp:
        cp.start()
    mine = dkv_ref[pl.ds(pl.multiple_of(m * R, R), R), :]
    dxo_ref[...] = dx_ref[...] + lax.dot_general(mine, wkv_ref[...], NT, preferred_element_type=F32)
    for i in (HL - 2, HL - 1):
        for j in range(2):
            o_copy(i, j, (i % 2) * 2 + j).wait()
            q_copy(i, j, (i % 2) * 2 + j).wait()
    for cp in k_cp:
        cp.wait()


def solution(mesh):
    tok = P(("data", "model"), None)

    def step(x, dy, w_query, w_key, w_value, w_out):
        wq = jnp.transpose(w_query, (1, 0, 2)).reshape(NP, 2, D, E)
        wo = w_out.reshape(HL * E, D)
        S = jax.ShapeDtypeStruct
        DMA = pltpu.SemaphoreType.DMA
        V = pltpu.VMEM
        xt, dyg, ot, dq, dkv, wkv, dxk, dxs = pl.pallas_call(
            attend_kernel,
            out_shape=[V((D, T), BF), V((T, D), BF), V((HL * E, T), BF), V((T, HL * E), BF), V((T, 2 * E), BF), V((D, 2 * E), BF), V((R, D), F32), V((R, D), F32)],
            in_specs=[ANY] * 6,
            out_specs=[VM] * 8,
            scratch_shapes=[
                V((T, D), BF), V((NP, D, 2 * E), BF), V((HL * E, D), BF), V((NP, T, 2 * E), F32), V((T, 2 * E), F32),
                V((2, T, N1), F32), V((2, N2, T), F32), V((HL * T, E), BF), V((HL * T, E), BF), V((HL * T, E), BF),
                V((4, R, HL * E), BF), V((4, T, 2 * E), F32), V((2, R, D), F32), V((2, R, D), F32), V((2, R, D), F32),
                DMA((2,)), DMA((2 + 2 * NQ + NY,)), DMA((2, NC)), DMA((2, NC)), DMA((2,)), DMA((2,)), DMA((2, NC)), DMA((2, NC)),
                DMA((3,)), DMA((3,)), DMA((NX,)), DMA((NX,)),
            ],
            compiler_params=pltpu.CompilerParams(collective_id=0, has_side_effects=True, vmem_limit_bytes=50 * 2**20),
            cost_estimate=pl.CostEstimate(flops=10**10, bytes_accessed=4 * 10**7, transcendentals=0),
            name="attend",
        )(x, dy, wq, w_key, w_value, wo)
        far = lax.ppermute(dxs, "model", [(0, 2), (2, 0), (1, 3), (3, 1)])
        dwq, dwo, dwk, dwv, dxo = pl.pallas_call(
            grads_kernel,
            out_shape=[S((NP, 2, D, E), F32), S((HL * E, D), F32), S((RQ, E), F32), S((RQ, E), F32), S((R, D), F32)],
            in_specs=[VM] * 7,
            out_specs=[ANY] * 4 + [VM],
            scratch_shapes=[V((NB, E, CW), F32), V((NB, 2, RQ, E), F32), V((2, RQ, E), F32), DMA((NB,)), DMA((NB,)), DMA((2,))],
            compiler_params=pltpu.CompilerParams(vmem_limit_bytes=24 * 2**20),
            cost_estimate=pl.CostEstimate(flops=4 * 10**10, bytes_accessed=8 * 10**7, transcendentals=0),
            name="grads",
        )(xt, dyg, ot, dq, dkv, wkv, dxk)
        dx = (dxo + far).astype(BF)
        dw_query = jnp.transpose(dwq.reshape(HL, D, E), (1, 0, 2))
        return dx, dw_query, dwk, dwv, dwo.reshape(HL, E, D)

    return jax.shard_map(step, mesh=mesh, in_specs=(tok, tok, P(None, "model", None), P(None, None), P(None, None), P("model", None, None)),
                         out_specs=(tok, P("data", "model", None), tok, tok, P(("data", "model"), None, None)), check_vma=False)
```

```python
import functools
import math
import jax
import jax.numpy as jnp
from jax import lax
from jax.experimental import pallas as pl
from jax.experimental.pallas import tpu as pltpu
from jax.sharding import PartitionSpec as P

MESH = pl.DeviceIdType.MESH
ANY = pl.BlockSpec(memory_space=pl.ANY)
VM = pl.BlockSpec(memory_space=pltpu.VMEM)
F32 = jnp.float32
BF = jnp.bfloat16
NT = (((1,), (1,)), ((), ()))
TN = (((0,), (0,)), ((), ()))

T, D, HL, E, R = 64, 6144, 12, 128, 16
NP = HL // 2
LEAD = 1
SIZES = ((1536, 1536, 1536, 1536), (2048, 2048, 1536, 512))
STARTS = tuple(tuple(sum(sz[:c]) for c in range(len(sz))) for sz in SIZES)
NY, NQ = len(SIZES[0]), len(SIZES[1])
NC = max(NY, NQ)
N1 = 512
N2 = 256
XB = N1 + N2
XS = (3, 3, 2)
NX = len(XS)
X0 = tuple(sum(XS[:c]) for c in range(NX))


def attend_kernel(x_ref, dy_ref, wq_ref, wk_ref, wv_ref, wo_ref,
                  xt_ref, dyg_ref, ot_ref, dq_ref, dkv_ref, wkv, dxk_ref, dxs_ref,
                  xg, wq, wo, qacc, kvacc, doacc, dot_acc, q_s, o_s, do_s, dqp, part, keep, send, got,
                  lsem, wsem, link_s, link_r, pair_s, pair_r, fwd_s, fwd_r, ex_s, ex_r, red_s, red_r):
    scale = 1.0 / math.sqrt(E)
    m = lax.axis_index("model")
    core, chip = m % 2, m // 2
    partner = chip * 2 + (1 - core)
    counter = (1 - chip) * 2 + core
    diag = (1 - chip) * 2 + (1 - core)
    own = pl.ds(pl.multiple_of(m * R, R), R)
    far = pl.ds(pl.multiple_of(counter * R, R), R)
    bufs = (dyg_ref, xg)

    def cols(a, c):
        return pl.ds(STARTS[a][c], SIZES[a][c])

    loads = [pltpu.make_async_copy(s, g.at[own], lsem.at[a]) for a, (s, g) in enumerate(((dy_ref, dyg_ref), (x_ref, xg)))]
    for cp in loads:
        cp.start()
    wkv_cp = [pltpu.make_async_copy(s, wkv.at[:, pl.ds(j * E, E)], wsem.at[j]) for j, s in enumerate((wk_ref, wv_ref))]
    wq_cp = [[pltpu.make_async_copy(wq_ref.at[:, j, cols(1, c), :], wq.at[:, cols(1, c), pl.ds(j * E, E)], wsem.at[2 + 2 * c + j])
              for j in range(2)] for c in range(NQ)]
    wo_cp = [pltpu.make_async_copy(wo_ref.at[:, cols(0, c)], wo.at[:, cols(0, c)], wsem.at[2 + 2 * NQ + c]) for c in range(NY)]
    for cp in wo_cp[:NY // 2]:
        cp.start(priority=1)

    barrier = pltpu.get_barrier_semaphore()
    for peer in (partner, counter, diag):
        pl.semaphore_signal(barrier, inc=1, device_id={"model": peer}, device_id_type=MESH)
    pl.semaphore_wait(barrier, 3)

    link, pair, fwd = [], [], []
    for a in range(2):
        g = bufs[a]
        loads[a].wait()
        link.append([pltpu.make_async_remote_copy(g.at[own, cols(a, c)], g.at[own, cols(a, c)], link_s.at[a, c], link_r.at[a, c],
                                                  device_id={"model": counter}, device_id_type=MESH) for c in range(len(SIZES[a]))])
        pair.append(pltpu.make_async_remote_copy(g.at[own], g.at[own], pair_s.at[a], pair_r.at[a],
                                                 device_id={"model": partner}, device_id_type=MESH))
        fwd.append([pltpu.make_async_remote_copy(g.at[far, cols(a, c)], g.at[far, cols(a, c)], fwd_s.at[a, c], fwd_r.at[a, c],
                                                 device_id={"model": partner}, device_id_type=MESH) for c in range(len(SIZES[a]))])
        for cp in link[a]:
            cp.start()
        pair[a].start()

    for cp in wo_cp[NY // 2:] + wkv_cp:
        cp.start(priority=1)

    def relay(i):
        a, c = (0, i) if i < NY else (1, i - NY)
        if c < len(SIZES[a]):
            link[a][c].wait_recv()
            fwd[a][c].start()

    for i in range(LEAD):
        relay(i)
    pair[0].wait_recv()
    for c in range(NY):
        relay(c + LEAD)
        fwd[0][c].wait_recv()
        wo_cp[c].wait()
        for cp in wq_cp[c] + (sum(wq_cp[NY:], []) if c == NY - 1 else []):
            cp.start(priority=1)
        dyc = dyg_ref[:, cols(0, c)]
        dyct = dyc.T
        for p in range(2):
            base = p * (N1 + N2)
            by_rows, by_cols = None, None
            for k in range(SIZES[0][c] // 256):
                ks = pl.ds(STARTS[0][c] + k * 256, 256)
                t1 = lax.dot_general(dyc[:, k * 256:(k + 1) * 256], wo[pl.ds(base, N1), ks], NT, preferred_element_type=F32)
                t2 = jnp.dot(wo[pl.ds(base + N1, N2), ks], dyct[k * 256:(k + 1) * 256, :], preferred_element_type=F32)
                by_rows = t1 if by_rows is None else by_rows + t1
                by_cols = t2 if by_cols is None else by_cols + t2
            if c == 0:
                doacc[p] = by_rows
                dot_acc[p] = by_cols
            else:
                doacc[p] += by_rows
                dot_acc[p] += by_cols
    for p in range(2):
        for j in range(6):
            rows = pl.ds((p * 6 + j) * T, T)
            if j < 4:
                do_s[rows, :] = doacc[p, :, j * E:(j + 1) * E].astype(BF)
            else:
                do_s[rows, :] = dot_acc[p, (j - 4) * E:(j - 3) * E, :].T.astype(BF)
    pair[1].wait_recv()
    for cp in wkv_cp:
        cp.wait()
    for c in range(NQ):
        relay(NY + c + LEAD)
        fwd[1][c].wait_recv()
        for cp in wq_cp[c]:
            cp.wait()
        xc = xg[:, cols(1, c)]
        for p in range(NP):
            part_q = jnp.dot(xc, wq[p, cols(1, c), :], preferred_element_type=F32)
            if c == 0:
                qacc[p] = part_q
            else:
                qacc[p] += part_q
        part_kv = jnp.dot(xc, wkv[cols(1, c), :], preferred_element_type=F32)
        if c == 0:
            kvacc[...] = part_kv
        else:
            kvacc[...] += part_kv
        xt_ref[cols(1, c), :] = xc.T
    kv = kvacc[...].astype(BF)
    keys, vals = kv[:, :E], kv[:, E:]
    for p in range(NP):
        qp = qacc[p].astype(BF)
        q_s[pl.ds(2 * p * T, T), :] = qp[:, :E]
        q_s[pl.ds((2 * p + 1) * T, T), :] = qp[:, E:]
    d_attn = do_s[...]
    s = lax.dot_general(q_s[...], keys, NT, preferred_element_type=F32) * scale
    d_probs = lax.dot_general(d_attn, vals, NT, preferred_element_type=F32)
    row = lax.broadcasted_iota(jnp.int32, (HL * T, T), 0) % T
    col = lax.broadcasted_iota(jnp.int32, (HL * T, T), 1)
    s = jnp.where(row >= col, s, -jnp.inf)
    e = jnp.exp(s - jnp.max(s, axis=-1, keepdims=True))
    p32 = e / jnp.sum(e, axis=-1, keepdims=True)
    pb = p32.astype(BF)
    ob = jnp.dot(pb, vals, preferred_element_type=F32).astype(BF)
    o_s[...] = ob
    row_dot = jnp.sum(d_attn.astype(F32) * ob.astype(F32), axis=-1, keepdims=True)
    g = (p32 * (d_probs - row_dot) * scale).astype(BF)
    part[0, :, E:] = lax.dot_general(pb, d_attn, TN, preferred_element_type=F32)
    part[0, :, :E] = lax.dot_general(g, q_s[...], TN, preferred_element_type=F32)
    d_query = jnp.dot(g, keys, preferred_element_type=F32).astype(BF)
    ex = [pltpu.make_async_remote_copy(part.at[0], part.at[i + 1], ex_s.at[i], ex_r.at[i], device_id={"model": peer}, device_id_type=MESH)
          for i, peer in enumerate((partner, counter, diag))]
    for cp in ex:
        cp.start()
    for h in range(HL):
        dqh = d_query[h * T:(h + 1) * T, :]
        dq_ref[:, pl.ds(h * E, E)] = dqh
        for r in range(4):
            slot = (r // 2 + chip) % 2 * 2 + (r % 2 + core) % 2
            dqp[slot, :, pl.ds(h * E, E)] = dqh[r * R:(r + 1) * R, :]
    lhs = dqp[...].reshape(T, HL * E)
    def xcols(c):
        return pl.ds(X0[c] * XB, XS[c] * XB)

    red = [pltpu.make_async_remote_copy(send.at[:, :, xcols(c)], got.at[:, :, xcols(c)], red_s.at[c], red_r.at[c],
                                        device_id={"model": partner}, device_id_type=MESH) for c in range(NX)]


    def dx_block(base):
        by_rows, by_cols = None, None
        for p in range(NP):
            ps = slice(p * 2 * E, (p + 1) * 2 * E)
            t1 = lax.dot_general(lhs[:, ps], wq[p, pl.ds(base, N1), :], NT, preferred_element_type=F32)
            t2 = lax.dot_general(wq[p, pl.ds(base + N1, N2), :], lhs[:, ps], NT, preferred_element_type=F32)
            by_rows = t1 if by_rows is None else by_rows + t1
            by_cols = t2 if by_cols is None else by_cols + t2
        by_cols = by_cols.T
        for k in range(4):
            dst, r = (send if k % 2 else keep), slice(k * R, (k + 1) * R)
            dst[k // 2, :, pl.ds(base, N1)] = by_rows[r, :]
            dst[k // 2, :, pl.ds(base + N1, N2)] = by_cols[r, :]

    def dx_sum(c):
        rows = xcols(c)
        red[c].wait_recv()
        dxk_ref[:, rows] = keep[0, :, rows] + got[0, :, rows]
        dxs_ref[:, rows] = keep[1, :, rows] + got[1, :, rows]

    for c in range(NX):
        for i in range(XS[c]):
            dx_block((X0[c] + i) * XB)
        if c >= 1:
            red[c - 1].start()
    for h in range(HL):
        ot_ref[pl.ds(h * E, E), :] = o_s[pl.ds(h * T, T), :].T
    red[NX - 1].start()
    for c in range(NX - 1):
        dx_sum(c)
    for cp in ex:
        cp.wait_recv()
    dkv_ref[...] = ((part[0] + part[1]) + (part[2] + part[3])).astype(BF)
    dx_sum(NX - 1)
    for a in range(2):
        pair[a].wait_send()
        for cp in link[a] + fwd[a]:
            cp.wait_send()
    for cp in ex + red:
        cp.wait_send()


NB = 4
CW = D // 2
RQ = D // 4


def grads_kernel(xt_ref, dyg_ref, ot_ref, dq_ref, dkv_ref, wkv_ref, dx_ref, dwq_ref, dwo_ref, dwk_ref, dwv_ref, dxo_ref,
                 bo, bq, bkv, osem, qsem, ksem):
    m = lax.axis_index("model")

    def o_copy(i, j, slot):
        return pltpu.make_async_copy(bo.at[slot], dwo_ref.at[pl.ds(pl.multiple_of(i * E, E), E), pl.ds(j * CW, CW)], osem.at[slot])

    def q_copy(i, j, slot):
        rows = pl.ds(pl.multiple_of((i % 2) * (2 * RQ) + j * RQ, RQ), RQ)
        return pltpu.make_async_copy(bq.at[slot], dwq_ref.at[i // 2, :, rows, :], qsem.at[slot])

    def body(i, carry):
        ot = ot_ref[pl.ds(pl.multiple_of(i * E, E), E), :]
        dq = dq_ref[:, pl.ds(pl.multiple_of((i // 2) * 2 * E, 2 * E), 2 * E)]
        for j in range(2):
            slot = (i % 2) * 2 + j

            @pl.when(i >= 2)
            def _():
                o_copy(i - 2, j, slot).wait()

            bo[slot] = jnp.dot(ot, dyg_ref[:, j * CW:(j + 1) * CW], preferred_element_type=F32)
            o_copy(i, j, slot).start()

            @pl.when(i >= 2)
            def _():
                q_copy(i - 2, j, slot).wait()

            rows = pl.ds(pl.multiple_of((i % 2) * (2 * RQ) + j * RQ, RQ), RQ)
            v = jnp.dot(xt_ref[rows, :], dq, preferred_element_type=F32)
            bq[slot, 0] = v[:, :E]
            bq[slot, 1] = v[:, E:]
            q_copy(i, j, slot).start()
        return carry

    lax.fori_loop(0, HL, body, 0)
    v = jnp.dot(xt_ref[pl.ds(pl.multiple_of(m * RQ, RQ), RQ), :], dkv_ref[...], preferred_element_type=F32)
    bkv[0] = v[:, :E]
    bkv[1] = v[:, E:]
    k_cp = [pltpu.make_async_copy(bkv.at[j], r, ksem.at[j]) for j, r in enumerate((dwk_ref, dwv_ref))]
    for cp in k_cp:
        cp.start()
    mine = dkv_ref[pl.ds(pl.multiple_of(m * R, R), R), :]
    dxo_ref[...] = dx_ref[...] + lax.dot_general(mine, wkv_ref[...], NT, preferred_element_type=F32)
    for i in (HL - 2, HL - 1):
        for j in range(2):
            o_copy(i, j, (i % 2) * 2 + j).wait()
            q_copy(i, j, (i % 2) * 2 + j).wait()
    for cp in k_cp:
        cp.wait()


def solution(mesh):
    tok = P(("data", "model"), None)

    def step(x, dy, w_query, w_key, w_value, w_out):
        wq = jnp.transpose(w_query, (1, 0, 2)).reshape(NP, 2, D, E)
        wo = w_out.reshape(HL * E, D)
        S = jax.ShapeDtypeStruct
        DMA = pltpu.SemaphoreType.DMA
        V = pltpu.VMEM
        xt, dyg, ot, dq, dkv, wkv, dxk, dxs = pl.pallas_call(
            attend_kernel,
            out_shape=[V((D, T), BF), V((T, D), BF), V((HL * E, T), BF), V((T, HL * E), BF), V((T, 2 * E), BF), V((D, 2 * E), BF), V((R, D), F32), V((R, D), F32)],
            in_specs=[ANY] * 6,
            out_specs=[VM] * 8,
            scratch_shapes=[
                V((T, D), BF), V((NP, D, 2 * E), BF), V((HL * E, D), BF), V((NP, T, 2 * E), F32), V((T, 2 * E), F32),
                V((2, T, N1), F32), V((2, N2, T), F32), V((HL * T, E), BF), V((HL * T, E), BF), V((HL * T, E), BF),
                V((4, R, HL * E), BF), V((4, T, 2 * E), F32), V((2, R, D), F32), V((2, R, D), F32), V((2, R, D), F32),
                DMA((2,)), DMA((2 + 2 * NQ + NY,)), DMA((2, NC)), DMA((2, NC)), DMA((2,)), DMA((2,)), DMA((2, NC)), DMA((2, NC)),
                DMA((3,)), DMA((3,)), DMA((NX,)), DMA((NX,)),
            ],
            compiler_params=pltpu.CompilerParams(collective_id=0, has_side_effects=True, vmem_limit_bytes=50 * 2**20),
            cost_estimate=pl.CostEstimate(flops=10**10, bytes_accessed=4 * 10**7, transcendentals=0),
            name="attend",
        )(x, dy, wq, w_key, w_value, wo)
        far = lax.ppermute(dxs, "model", [(0, 2), (2, 0), (1, 3), (3, 1)])
        dwq, dwo, dwk, dwv, dxo = pl.pallas_call(
            grads_kernel,
            out_shape=[S((NP, 2, D, E), F32), S((HL * E, D), F32), S((RQ, E), F32), S((RQ, E), F32), S((R, D), F32)],
            in_specs=[VM] * 7,
            out_specs=[ANY] * 4 + [VM],
            scratch_shapes=[V((NB, E, CW), F32), V((NB, 2, RQ, E), F32), V((2, RQ, E), F32), DMA((NB,)), DMA((NB,)), DMA((2,))],
            compiler_params=pltpu.CompilerParams(vmem_limit_bytes=24 * 2**20),
            cost_estimate=pl.CostEstimate(flops=4 * 10**10, bytes_accessed=8 * 10**7, transcendentals=0),
            name="grads",
        )(xt, dyg, ot, dq, dkv, wkv, dxk)
        dx = (dxo + far).astype(BF)
        dw_query = jnp.transpose(dwq.reshape(HL, D, E), (1, 0, 2))
        return dx, dw_query, dwk, dwv, dwo.reshape(HL, E, D)

    return jax.shard_map(step, mesh=mesh, in_specs=(tok, tok, P(None, "model", None), P(None, None), P(None, None), P("model", None, None)),
                         out_specs=(tok, P("data", "model", None), tok, tok, P(("data", "model"), None, None)), check_vma=False)
```
